32 devices in a mesh: seq: 8 (over y, x, core), tp: 4 (over z).
Axes of the slice: x: 2, y: 2, z: 4, core: 2. Of those that a mesh axis runs over, the one named last changes fastest.
Arguments:
- x_input: bfloat16 [8192, 8192], P('seq', 'tp'), may hold values from -6 to 6
- bc_input: bfloat16 [8192, 2048], P('seq', 'tp'), may hold values from -3 to 3
- z_gate: bfloat16 [8192, 8192], P('seq', 'tp'), may hold values from -6 to 6
- dt_input: bfloat16 [128, 8192], P('tp', 'seq'), may hold values from -3.4 to 3.4
- conv_weight_x: bfloat16 [4, 8192], P(None, 'tp'), may hold values from -3 to 3
- conv_weight_bc: bfloat16 [4, 2048], P(None, 'tp'), may hold values from -3 to 3
- conv_bias_x: float32 [8192], P('tp'), may hold values from -3 to 3
- conv_bias_bc: float32 [2048], P('tp'), may hold values from -3 to 3
- dt_bias: float32 [128], P('tp'), may hold values from -1 to 0.5
- decay_log: float32 [128], P('tp'), may hold values from -12 to -3.3
- skip_scale: float32 [128], P('tp'), may hold values from 0.5 to 2
- norm_gain: float32 [8192], P('tp'), may hold values from 0.25 to 1.75
Outputs:
- layer_out: bfloat16 [8192, 8192], P('seq', 'tp')
The draws below stay inside these ranges and needn't reach their ends.
All inputs are finite; a program needn't handle non-finite values.
Results may differ from the reference program's by a relative error of at most 0.0048.
Values may be sent and summed in bfloat16 or wider, within the bound.
A program may use at most 128 MiB of HBM per device.

```python
import jax
import jax.numpy as jnp
from jax import lax

HEADS = 128
HEAD_DIM = 64
STATE = 128
GROUPS = 8
SPAN = 256
TOK_DEV = 1024
DI = 8192
LENGTH = 8192


def smooth_rows(key, rows, cols, knot):
    shift_key, knot_key = jax.random.split(key)
    count = rows // knot + 2
    knots = jax.random.normal(knot_key, (count, cols), dtype=jnp.float32)
    frac = (jnp.arange(knot, dtype=jnp.float32) / knot)[None, :, None]
    field = (knots[:-1][:, None, :] * (1.0 - frac) + knots[1:][:, None, :] * frac).reshape((count - 1) * knot, cols)
    offset = jax.random.randint(shift_key, (), 0, knot)
    return lax.dynamic_slice_in_dim(field, offset, rows, 0)


def draw_x_input(key, part):
    noise_key, field_key = jax.random.split(jax.random.fold_in(key, 7))
    field = smooth_rows(field_key, LENGTH, DI, SPAN)
    noise = 0.6 * jax.random.normal(noise_key, (LENGTH, DI))
    total = noise + 0.9 * field
    return jnp.clip(total, -6.0, 6.0).astype(jnp.float32).astype(jnp.bfloat16)


def draw_bc_input(key, part):
    noise_key, field_key = jax.random.split(jax.random.fold_in(key, 11))
    width = 2 * GROUPS * STATE
    field = smooth_rows(field_key, LENGTH, width, SPAN)
    noise = 0.3 * jax.random.normal(noise_key, (LENGTH, width))
    total = noise + 0.5 * field
    return jnp.clip(total, -3.0, 3.0).astype(jnp.float32).astype(jnp.bfloat16)


def draw_dt_input(key, part):
    noise_key, shift_key = jax.random.split(jax.random.fold_in(key, 23))
    blocks = LENGTH // TOK_DEV
    offsets = jax.random.uniform(shift_key, (HEADS, blocks, 1), minval=-0.8, maxval=0.8)
    noise = jnp.clip(0.5 * jax.random.normal(noise_key, (HEADS, blocks, TOK_DEV)), -2.5, 2.5)
    return (offsets + noise).reshape(HEADS, LENGTH).astype(jnp.float32).astype(jnp.bfloat16)


def draw_decay_log(key, part):
    kind_key, slow_key, other_key = jax.random.split(jax.random.fold_in(key, 41), 3)
    picker = jax.random.uniform(kind_key, (HEADS,))
    slow_heads = picker < 0.5
    slow_log = jax.random.uniform(slow_key, (HEADS,), minval=jnp.log(0.3), maxval=jnp.log(2.0)) - jnp.log(1.0 * LENGTH)
    other_log = jax.random.uniform(other_key, (HEADS,), minval=jnp.log(2.0 / LENGTH), maxval=jnp.log(1.0 / 30.0))
    return jnp.where(slow_heads, slow_log, other_log).astype(jnp.float32)


def block_scale(stream_key, shape, cuts, smallest, largest):
    level, own = 1.0, jax.random.fold_in(stream_key, 6)
    for position, blocks in cuts:
        draws = jnp.exp(jax.random.uniform(jax.random.fold_in(own, position), (blocks,), jnp.float32, smallest / len(cuts), largest / len(cuts)))
        level = level * jnp.repeat(draws, shape[position] // blocks).reshape([-1 if axis == position else 1 for axis in range(len(shape))])
    return level


def gaussian(own_key, dims, scale, bound, cuts=(), kind=jnp.bfloat16):
    entries = jax.random.normal(own_key, dims, jnp.float32) * scale
    if len(cuts) > 0:
        entries = block_scale(own_key, dims, cuts, -0.22, 0.18) * entries
    return jnp.clip(entries, min=-bound, max=bound).astype(kind)


def setup_inputs(seed: int = 0) -> dict:
    streams_of = jax.random.split(jax.random.key(seed), 13)
    x_input = draw_x_input(jax.random.fold_in(streams_of[12], 71), 0)
    bc_input = draw_bc_input(jax.random.fold_in(streams_of[12], 71), 0)
    z_gate = gaussian(streams_of[2], (LENGTH, DI), 1.0, 6.0, ((0, 8), (1, 4)))
    dt_input = draw_dt_input(jax.random.fold_in(streams_of[12], 71), 0)
    conv_weight_x = gaussian(streams_of[4], (4, DI), 4 ** -0.5, 3.0, ((1, 4),))
    conv_weight_bc = gaussian(streams_of[5], (4, 2 * GROUPS * STATE), 4 ** -0.5, 3.0, ((1, 4),))
    conv_bias_x = gaussian(streams_of[6], (DI,), 0.5, 3.0, ((0, 4),), jnp.float32)
    conv_bias_bc = gaussian(streams_of[7], (2 * GROUPS * STATE,), 0.5, 3.0, ((0, 4),), jnp.float32)
    dt_bias = jnp.clip(-1.0 + 1.5 * jax.random.uniform(streams_of[8], (HEADS,), jnp.float32) ** block_scale(streams_of[8], (HEADS,), ((0, 4),), -0.2, 0.2), -1.0, 0.5)
    decay_log = draw_decay_log(jax.random.fold_in(streams_of[12], 71), 0)
    skip_scale = jnp.clip(0.5 + 1.5 * jax.random.uniform(streams_of[10], (HEADS,), jnp.float32) ** block_scale(streams_of[10], (HEADS,), ((0, 4),), -0.2, 0.2), 0.5, 2.0)
    norm_gain = jnp.clip(1.0 + 0.15 * jax.random.normal(streams_of[11], (DI,), jnp.float32), 0.25, 1.75)
    return {"x_input": x_input, "bc_input": bc_input, "z_gate": z_gate, "dt_input": dt_input, "conv_weight_x": conv_weight_x, "conv_weight_bc": conv_weight_bc, "conv_bias_x": conv_bias_x, "conv_bias_bc": conv_bias_bc, "dt_bias": dt_bias, "decay_log": decay_log, "skip_scale": skip_scale, "norm_gain": norm_gain}


epsilon = 1e-05

def causal_conv(padded, weight, bias_row):
    length = padded.shape[0] - 3
    total = jnp.zeros((length, padded.shape[1]), jnp.float32) + bias_row.astype(jnp.float32)[None, :]
    for offset in range(4):
        total = total + padded[offset:offset + length].astype(jnp.float32) * weight[offset].astype(jnp.float32)[None, :]
    return jax.nn.silu(total).astype(jnp.bfloat16)

def span_local(x_block, bc_block, dt_block, decay_block):
    block_len = x_block.shape[0]
    heads = x_block.shape[1]
    groups = bc_block.shape[1]
    group_heads = heads // groups
    cum_decay = jnp.cumsum(decay_block, axis=1)
    b_part = bc_block[:, :, 0, :].astype(jnp.float32)
    c_part = bc_block[:, :, 1, :].astype(jnp.float32)
    scores = jnp.einsum('ign,jgn->gij', c_part, b_part)
    causal = jnp.arange(block_len)[:, None] >= jnp.arange(block_len)[None, :]
    spread = jnp.where(causal[None], cum_decay[:, :, None] - cum_decay[:, None, :], -jnp.inf)
    weights = jnp.exp(spread) * dt_block[:, None, :]
    mixing = (weights.reshape(groups, group_heads, block_len, block_len) * scores[:, None]).reshape(heads, block_len, block_len).astype(jnp.bfloat16)
    mixing = lax.optimization_barrier(mixing)
    y_intra = jnp.einsum('hij,jhp->ihp', mixing.astype(jnp.float32), x_block.astype(jnp.float32))
    to_end = jnp.exp(cum_decay[:, -1:] - cum_decay) * dt_block
    weighted = (to_end.reshape(groups, group_heads, block_len)[:, :, :, None] * b_part.transpose(1, 0, 2)[:, None]).reshape(heads, block_len, b_part.shape[2]).astype(jnp.bfloat16)
    weighted = lax.optimization_barrier(weighted)
    span_state = jnp.einsum('hjn,jhp->hnp', weighted.astype(jnp.float32), x_block.astype(jnp.float32))
    return (y_intra, span_state, cum_decay)

def state_out(c_part, cum_decay, start):
    groups = c_part.shape[1]
    heads = start.shape[0]
    grouped = start.reshape(groups, heads // groups, start.shape[1], start.shape[2])
    product = jnp.einsum('ign,grnp->igrp', c_part.astype(jnp.float32), grouped.astype(jnp.float32))
    product = product.reshape(c_part.shape[0], heads, start.shape[2])
    return jnp.exp(cum_decay).T[:, :, None] * product

def reference(x_input, bc_input, z_gate, dt_input, conv_weight_x, conv_weight_bc, conv_bias_x, conv_bias_bc, dt_bias, decay_log, skip_scale, norm_gain):
    x_conv = causal_conv(jnp.concatenate([jnp.zeros((3, x_input.shape[1]), x_input.dtype), x_input], 0), conv_weight_x, conv_bias_x)
    bc_conv = causal_conv(jnp.concatenate([jnp.zeros((3, bc_input.shape[1]), bc_input.dtype), bc_input], 0), conv_weight_bc, conv_bias_bc)
    step_size = jax.nn.softplus(dt_input.astype(jnp.float32) + dt_bias[:, None])
    log_decay = -jnp.exp(decay_log)[:, None] * step_size
    blocks = LENGTH // SPAN
    x_blocks = x_conv.reshape(blocks, SPAN, HEADS, HEAD_DIM)
    bc_blocks = bc_conv.reshape(blocks, SPAN, GROUPS, 2, STATE)
    dt_blocks = step_size.reshape(HEADS, blocks, SPAN).transpose(1, 0, 2)
    decay_blocks = log_decay.reshape(HEADS, blocks, SPAN).transpose(1, 0, 2)

    def advance(carried, pieces):
        x_block, bc_block, dt_block, decay_block = pieces
        y_intra, span_state, cum_decay = span_local(x_block, bc_block, dt_block, decay_block)
        start = lax.optimization_barrier(carried.astype(jnp.bfloat16))
        mixed_block = y_intra + state_out(bc_block[:, :, 1, :], cum_decay, start)
        carried = jnp.exp(cum_decay[:, -1])[:, None, None] * carried + span_state
        return (carried, mixed_block)
    initial = jnp.zeros((HEADS, STATE, HEAD_DIM), jnp.float32)
    _, mixed = lax.scan(advance, initial, (x_blocks, bc_blocks, dt_blocks, decay_blocks))
    mixed = mixed.reshape(LENGTH, HEADS, HEAD_DIM) + skip_scale[None, :, None] * x_conv.reshape(LENGTH, HEADS, HEAD_DIM).astype(jnp.float32)
    gated = mixed.reshape(LENGTH, DI) * jax.nn.silu(z_gate.astype(jnp.float32))
    mean_square = lax.optimization_barrier(jnp.mean(gated * gated, axis=1))
    return (gated * lax.rsqrt(mean_square + epsilon)[:, None] * norm_gain[None, :]).astype(jnp.bfloat16)
```

```python
import functools

import jax
import jax.numpy as jnp
from jax import lax
from jax.experimental import pallas as pl
from jax.experimental.pallas import tpu as pltpu
from jax.sharding import PartitionSpec as P

HEAD_DIM = 64
STATE = 128
SPAN = 256
LANES = 256
PIECE = 64
RIM = 16
DECAY_ROWS = 16

epsilon = 1e-05

F32 = jnp.float32
BF16 = jnp.bfloat16
MESH = pl.DeviceIdType.MESH


def silu(value):
    half = 0.5 * value
    return half + half * jnp.tanh(half)


def conv_piece(buffer, row, lanes, taps):
    raw = buffer[pl.ds(row, PIECE + RIM), lanes].astype(F32)
    total = raw[RIM - 3 : RIM - 3 + PIECE] * taps[0:1, lanes] + taps[4:5, lanes]
    for k in range(1, 4):
        total = total + raw[RIM - 3 + k : RIM - 3 + k + PIECE] * taps[k : k + 1, lanes]
    return silu(total).astype(BF16)


def two_rows(row):
    high = row.astype(BF16).astype(F32)
    low = row - high
    width = row.shape[1]
    return jnp.concatenate(
        [jnp.broadcast_to(high, (8, width)), jnp.broadcast_to(low, (8, width))], 0
    ).astype(BF16)


def read_row(pair):
    wide = pair.astype(F32)
    return wide[0:1] + wide[8:9]


def scan_kernel(
    n_seq,
    n_tp,
    steps,
    x_hbm,
    bc_hbm,
    z_hbm,
    dt_ref,
    taps_x,
    taps_bc,
    head_ref,
    gated_hbm,
    total_ref,
    xb,
    bcb,
    zb,
    xc,
    xp,
    bcc,
    tt,
    rn,
    rp,
    dec,
    pre,
    u,
    ls,
    own,
    p_buf,
    q_buf,
    gb,
    sm,
    skip_row,
    sq,
    i_buf,
    e_buf,
    d_buf,
    sa,
    ra,
    sk,
    rk,
    se,
    re,
    ss,
    rs,
    in_sem,
    out_sem,
    send_sem,
    recv_sem,
):
    tokens, width = x_hbm.shape
    heads = dt_ref.shape[0]
    groups = bc_hbm.shape[1] // (2 * STATE)
    group_width = width // groups
    half_width = width // 2
    blocks = tokens // SPAN
    chunks = width // LANES
    half_chunks = half_width // LANES
    seq = lax.axis_index("seq")
    tp = lax.axis_index("tp")
    chip, core = seq // 2, seq % 2
    partner = seq + 1 - 2 * core
    chips = n_seq // 2

    def rows_of(b):
        return pl.ds(b * SPAN, SPAN)

    loads = []
    for b in range(blocks):
        loads.append(
            (
                pltpu.make_async_copy(
                    bc_hbm.at[rows_of(b), :],
                    bcb.at[pl.ds(RIM + b * SPAN, SPAN), :],
                    in_sem.at[0, b],
                ),
                pltpu.make_async_copy(
                    x_hbm.at[rows_of(b), :],
                    xb.at[pl.ds(RIM + b * SPAN, SPAN), :],
                    in_sem.at[1, b],
                ),
                pltpu.make_async_copy(z_hbm.at[rows_of(b), :], zb.at[rows_of(b), :], in_sem.at[2, b]),
            )
        )
    for b in range(blocks):
        loads[b][0].start()
        loads[b][1].start()
    for b in range(blocks):
        loads[b][2].start()

    def at_seq(place):
        return {"seq": place, "tp": tp}

    barrier = pltpu.get_barrier_semaphore()
    sources = [at_seq((seq + n_seq - 1) % n_seq), at_seq(partner)]
    for j in range(steps):
        sources.append(at_seq(((chip + chips - 2**j) % chips) * 2 + core))
    for k in range(1, n_tp):
        sources.append({"seq": seq, "tp": (tp + n_tp - k) % n_tp})
    for source in sources:
        pl.semaphore_signal(barrier, inc=1, device_id=source, device_id_type=MESH)
    pl.semaphore_wait(barrier, len(sources))

    def remote(source, target, slot, device):
        return pltpu.make_async_remote_copy(
            src_ref=source,
            dst_ref=target,
            send_sem=send_sem.at[slot],
            recv_sem=recv_sem.at[slot],
            device_id=device,
            device_id_type=MESH,
        )

    following = at_seq((seq + 1) % n_seq)
    last_rows = pl.ds(tokens - RIM, RIM)
    rim_x = remote(x_hbm.at[last_rows, :], xb.at[pl.ds(0, RIM), :], 0, following)
    rim_bc = remote(bc_hbm.at[last_rows, :], bcb.at[pl.ds(0, RIM), :], 1, following)
    rim_x.start()
    rim_bc.start()

    row_id = lax.broadcasted_iota(jnp.int32, (256, LANES), 0) % 128
    lane_id = lax.broadcasted_iota(jnp.int32, (256, LANES), 1) // HEAD_DIM
    for c in range(chunks):
        lanes = pl.ds(c * LANES, LANES)
        head = lane_id + c * (LANES // HEAD_DIM)
        rn[:, lanes] = jnp.where(row_id == head, 1.0, 0.0).astype(BF16)
        rp[:, lanes] = jnp.where(row_id == head + heads, 1.0, 0.0).astype(BF16)
    upper = jnp.where(
        lax.broadcasted_iota(jnp.int32, (SPAN, SPAN), 0)
        <= lax.broadcasted_iota(jnp.int32, (SPAN, SPAN), 1),
        1.0,
        0.0,
    )
    rate = -jnp.exp(head_ref[:, 1:2])
    for b in range(blocks):
        raw = dt_ref[:, rows_of(b)].astype(F32) + head_ref[:, 0:1]
        step = jnp.maximum(raw, 0.0) + jnp.log(1.0 + jnp.exp(-jnp.abs(raw)))
        cum = jnp.dot(
            rate * step, upper, precision=lax.Precision.HIGHEST, preferred_element_type=F32
        )
        parts = [jnp.exp(-cum) * step, jnp.exp(cum)]
        if 2 * heads < 128:
            parts.append(jnp.zeros((128 - 2 * heads, SPAN), F32))
        turned = jnp.concatenate(parts, 0).T
        high = turned.astype(BF16)
        tt[rows_of(b), 0:128] = high
        tt[rows_of(b), 128:256] = (turned - high.astype(F32)).astype(BF16)
    skip_wide = jnp.broadcast_to(head_ref[:, 2:3], (heads, 128)).T[0:16]
    skip_high = skip_wide.astype(BF16)
    skip_low = (skip_wide - skip_high.astype(F32)).astype(BF16)
    for c in range(chunks):
        lanes = pl.ds(c * LANES, LANES)
        skip_row[:, lanes] = (
            jnp.dot(skip_high, rn[0:heads, lanes], preferred_element_type=F32)
            + jnp.dot(skip_low, rn[0:heads, lanes], preferred_element_type=F32)
        )[0:8]
        running = jnp.ones((1, LANES), F32)
        for b in range(blocks):
            ends = jnp.dot(
                tt[pl.ds((b + 1) * SPAN - 16, 16), :], rp[:, lanes], preferred_element_type=F32
            )
            dec[b : b + 1, lanes] = ends[15:16]
            pre[b : b + 1, lanes] = running
            running = running * ends[15:16]
        pre[blocks : blocks + 1, lanes] = running

    def conv_block(b):
        def bc_piece(r, carry):
            row = pl.multiple_of(b * SPAN + r * PIECE, PIECE)
            for c in range(2 * groups * STATE // LANES):
                lanes = pl.ds(c * LANES, LANES)
                bcc[pl.ds(row, PIECE), lanes] = conv_piece(bcb, row, lanes, taps_bc)
            return carry

        lax.fori_loop(0, SPAN // PIECE, bc_piece, 0)

        def x_chunk(c, carry):
            lanes = pl.ds(pl.multiple_of(c * LANES, LANES), LANES)
            scale = jnp.dot(tt[rows_of(b), :], rn[:, lanes], preferred_element_type=F32)
            for r in range(SPAN // PIECE):
                row = b * SPAN + r * PIECE
                conv = conv_piece(xb, row, lanes, taps_x)
                xc[pl.ds(row, PIECE), lanes] = conv
                xp[pl.ds(row, PIECE), lanes] = (
                    conv.astype(F32) * scale[r * PIECE : (r + 1) * PIECE]
                ).astype(BF16)
            group = c // (group_width // LANES)
            b_part = bcc[rows_of(b), pl.ds(pl.multiple_of(group * 2 * STATE, STATE), STATE)]
            u[b, :, lanes] = lax.dot_general(
                b_part, xp[rows_of(b), lanes], (((0,), (0,)), ((), ())), preferred_element_type=F32
            )
            return carry

        lax.fori_loop(0, chunks, x_chunk, 0)

    loads[0][0].wait()
    loads[0][1].wait()
    for b in range(1, blocks):
        loads[b][0].wait()
        loads[b][1].wait()
        conv_block(b)
    rim_x.wait()
    rim_bc.wait()
    inner = (seq > 0).astype(F32)
    xb[0:RIM, :] = (xb[0:RIM, :].astype(F32) * inner).astype(BF16)
    bcb[0:RIM, :] = (bcb[0:RIM, :].astype(F32) * inner).astype(BF16)
    conv_block(0)

    def carry_chunk(c, carry):
        lanes = pl.ds(pl.multiple_of(c * LANES, LANES), LANES)
        half = c // half_chunks
        local = pl.ds(pl.multiple_of((c % half_chunks) * LANES, LANES), LANES)
        state = jnp.zeros((STATE, LANES), F32)
        for b in range(blocks):
            ls[b, :, lanes] = state.astype(BF16)
            state = dec[b : b + 1, lanes] * (state + u[b, :, lanes])
        own[:, lanes] = state
        sa[half, 0:STATE, local] = state.astype(BF16)
        sa[half, STATE : STATE + DECAY_ROWS, local] = two_rows(pre[blocks : blocks + 1, lanes])
        return carry

    lax.fori_loop(0, chunks, carry_chunk, 0)
    pair = remote(sa, ra, 2, at_seq(partner))
    pair.start()

    causal = lax.broadcasted_iota(jnp.int32, (SPAN, SPAN), 0) >= lax.broadcasted_iota(
        jnp.int32, (SPAN, SPAN), 1
    )

    def intra_block(b):
        loads[b][2].wait()
        for g in range(groups):
            b_part = bcc[rows_of(b), pl.ds(g * 2 * STATE, STATE)]
            c_part = bcc[rows_of(b), pl.ds(g * 2 * STATE + STATE, STATE)]
            scores = lax.dot_general(
                c_part, b_part, (((1,), (1,)), ((), ())), preferred_element_type=F32
            )
            sm[g] = jnp.where(causal, scores, 0.0).astype(BF16)

        def chunk(c, carry):
            lanes = pl.ds(pl.multiple_of(c * LANES, LANES), LANES)
            group = c // (group_width // LANES)
            c_part = bcc[
                rows_of(b), pl.ds(pl.multiple_of(group * 2 * STATE + STATE, STATE), STATE)
            ]
            y = jnp.dot(sm[group], xp[rows_of(b), lanes], preferred_element_type=F32)
            y = y + jnp.dot(c_part, ls[b, :, lanes], preferred_element_type=F32)
            scale = jnp.dot(tt[rows_of(b), :], rp[:, lanes], preferred_element_type=F32)
            for r in range(SPAN // PIECE):
                part = slice(r * PIECE, (r + 1) * PIECE)
                rows = pl.ds(b * SPAN + r * PIECE, PIECE)
                gate = silu(zb[rows, lanes].astype(F32))
                mixed = scale[part] * y[part] + skip_row[0:1, lanes] * xc[rows, lanes].astype(F32)
                p_buf[rows, lanes] = mixed * gate
                q_buf[rows, lanes] = scale[part] * gate
            return carry

        lax.fori_loop(0, chunks, chunk, 0)

    flag = core.astype(F32)

    def joined_chunk(j, carry):
        local = pl.ds(pl.multiple_of(j * LANES, LANES), LANES)
        lanes = pl.ds(pl.multiple_of(core * half_width + j * LANES, LANES), LANES)
        mine, mine_decay = own[:, lanes], pre[blocks : blocks + 1, lanes]
        other = ra[core, 0:STATE, local].astype(F32)
        other_decay = read_row(ra[core, STATE : STATE + DECAY_ROWS, local])
        joined = (1.0 - flag) * (other_decay * mine + other) + flag * (mine_decay * other + mine)
        decay = mine_decay * other_decay
        i_buf[:, local] = joined
        e_buf[:, local] = jnp.zeros_like(joined)
        d_buf[0:1, local] = decay
        d_buf[1:2, local] = jnp.ones_like(decay)
        sk[0, 0:STATE, local] = joined.astype(BF16)
        sk[0, STATE : STATE + DECAY_ROWS, local] = two_rows(decay)
        return carry

    def double(step):
        valid = (chip >= 2**step).astype(F32)

        def body(j, carry):
            local = pl.ds(pl.multiple_of(j * LANES, LANES), LANES)
            got = rk[step, 0:STATE, local].astype(F32) * valid
            got_decay = (
                read_row(rk[step, STATE : STATE + DECAY_ROWS, local]) * valid + (1.0 - valid)
            )
            e_decay = d_buf[1:2, local]
            earlier = e_decay * got + e_buf[:, local]
            e_buf[:, local] = earlier
            d_buf[1:2, local] = e_decay * got_decay
            if step < steps - 1:
                i_decay = d_buf[0:1, local]
                joined = i_decay * got + i_buf[:, local]
                decay = i_decay * got_decay
                i_buf[:, local] = joined
                d_buf[0:1, local] = decay
                sk[step + 1, 0:STATE, local] = joined.astype(BF16)
                sk[step + 1, STATE : STATE + DECAY_ROWS, local] = two_rows(decay)
            else:
                se[:, local] = earlier.astype(BF16)
            return carry

        lax.fori_loop(0, half_chunks, body, 0)

    def hop(step):
        target = at_seq(((chip + 2**step) % chips) * 2 + core)
        return remote(sk.at[step], rk.at[step], 4 + step, target)

    done = 0
    intra_block(done)
    done += 1
    pair.wait()
    lax.fori_loop(0, half_chunks, joined_chunk, 0)
    for step in range(steps):
        moving = hop(step)
        moving.start()
        if done < blocks:
            intra_block(done)
            done += 1
        moving.wait()
        double(step)
    back = remote(se, re, 3, at_seq(partner))
    back.start()
    while done < blocks:
        intra_block(done)
        done += 1
    back.wait()

    def incoming_chunk(c, carry):
        lanes = pl.ds(pl.multiple_of(c * LANES, LANES), LANES)
        half = c // half_chunks
        local = pl.ds(pl.multiple_of((c % half_chunks) * LANES, LANES), LANES)
        here = (half == core).astype(F32)
        state = here * e_buf[:, local] + (1.0 - here) * re[:, local].astype(F32)
        other = ra[half, 0:STATE, local].astype(F32)
        other_decay = read_row(ra[half, STATE : STATE + DECAY_ROWS, local])
        own[:, lanes] = (1.0 - flag) * state + flag * (other_decay * state + other)
        return carry

    lax.fori_loop(0, chunks, incoming_chunk, 0)

    stores = []
    for b in range(blocks):
        sq[...] = jnp.zeros_like(sq)

        def final(c, carry):
            lanes = pl.ds(pl.multiple_of(c * LANES, LANES), LANES)
            group = c // (group_width // LANES)
            c_part = bcc[
                rows_of(b), pl.ds(pl.multiple_of(group * 2 * STATE + STATE, STATE), STATE)
            ]
            start = (own[:, lanes] * pre[b : b + 1, lanes]).astype(BF16)
            y = jnp.dot(c_part, start, preferred_element_type=F32)
            for r in range(SPAN // PIECE):
                part = slice(r * PIECE, (r + 1) * PIECE)
                rows = pl.ds(b * SPAN + r * PIECE, PIECE)
                gated = p_buf[rows, lanes] + q_buf[rows, lanes] * y[part]
                gb[rows, lanes] = gated.astype(BF16)
                square = gated * gated
                total = square[:, 0:128]
                for i in range(1, LANES // 128):
                    total = total + square[:, i * 128 : (i + 1) * 128]
                sq[pl.ds(r * PIECE, PIECE), :] += total
            return carry

        lax.fori_loop(0, chunks, final, 0)
        ss[:, pl.ds(b * SPAN, SPAN)] = jnp.broadcast_to(
            jnp.sum(sq[...].T, axis=0, keepdims=True), (8, SPAN)
        )
        store = pltpu.make_async_copy(gb.at[rows_of(b), :], gated_hbm.at[rows_of(b), :], out_sem.at[b])
        store.start()
        stores.append(store)

    shares = []
    for k in range(1, n_tp):
        share = remote(
            ss, rs.at[k - 1], 3 + steps + k, {"seq": seq, "tp": (tp + k) % n_tp}
        )
        share.start()
        shares.append(share)
    for share in shares:
        share.wait()
    total = ss[...]
    for k in range(n_tp - 1):
        total = total + rs[k]
    total_ref[...] = lax.rsqrt(total * (1.0 / (width * n_tp)) + epsilon)
    for store in stores:
        store.wait()


def scale_kernel(gated_ref, factor_ref, gain_ref, out_ref):
    column = factor_ref[...].T[:, 0:1]
    for r in range(0, gated_ref.shape[0], PIECE):
        rows = pl.ds(r, PIECE)
        wide = gated_ref[rows, :].astype(F32)
        out_ref[rows, :] = (wide * column[r : r + PIECE] * gain_ref[...]).astype(BF16)


def local(
    n_seq,
    n_tp,
    x_input,
    bc_input,
    z_gate,
    dt_input,
    conv_weight_x,
    conv_weight_bc,
    conv_bias_x,
    conv_bias_bc,
    dt_bias,
    decay_log,
    skip_scale,
    norm_gain,
):
    tokens, width = x_input.shape
    bc_width = bc_input.shape[1]
    heads = dt_input.shape[0]
    groups = bc_width // (2 * STATE)
    blocks = tokens // SPAN
    half_width = width // 2
    steps = max(1, (n_seq // 2 - 1).bit_length())

    def taps(weight, bias):
        return jnp.concatenate(
            [weight.astype(F32), bias[None, :], jnp.zeros((3, bias.shape[0]), F32)], 0
        )

    none = jnp.zeros_like(dt_bias)
    head_rows = jnp.stack([dt_bias, decay_log, skip_scale, none, none, none, none, none], axis=1)
    whole = pl.BlockSpec(memory_space=pltpu.VMEM)
    anywhere = pl.BlockSpec(memory_space=pl.ANY)
    message = STATE + DECAY_ROWS
    copies = 4 + steps + n_tp - 1
    gated, factor = pl.pallas_call(
        functools.partial(scan_kernel, n_seq, n_tp, steps),
        out_shape=(
            jax.ShapeDtypeStruct((tokens, width), BF16),
            jax.ShapeDtypeStruct((8, tokens), F32),
        ),
        in_specs=[anywhere] * 3 + [whole] * 4,
        out_specs=(anywhere, whole),
        scratch_shapes=[
            pltpu.VMEM((RIM + tokens, width), BF16),
            pltpu.VMEM((RIM + tokens, bc_width), BF16),
            pltpu.VMEM((tokens, width), BF16),
            pltpu.VMEM((tokens, width), BF16),
            pltpu.VMEM((tokens, width), BF16),
            pltpu.VMEM((tokens, bc_width), BF16),
            pltpu.VMEM((tokens, 256), BF16),
            pltpu.VMEM((256, width), BF16),
            pltpu.VMEM((256, width), BF16),
            pltpu.VMEM((8, width), F32),
            pltpu.VMEM((8, width), F32),
            pltpu.VMEM((blocks, STATE, width), F32),
            pltpu.VMEM((blocks, STATE, width), BF16),
            pltpu.VMEM((STATE, width), F32),
            pltpu.VMEM((tokens, width), F32),
            pltpu.VMEM((tokens, width), F32),
            pltpu.VMEM((tokens, width), BF16),
            pltpu.VMEM((groups, SPAN, SPAN), BF16),
            pltpu.VMEM((8, width), F32),
            pltpu.VMEM((SPAN, 128), F32),
            pltpu.VMEM((STATE, half_width), F32),
            pltpu.VMEM((STATE, half_width), F32),
            pltpu.VMEM((8, half_width), F32),
            pltpu.VMEM((2, message, half_width), BF16),
            pltpu.VMEM((2, message, half_width), BF16),
            pltpu.VMEM((steps, message, half_width), BF16),
            pltpu.VMEM((steps, message, half_width), BF16),
            pltpu.VMEM((STATE, half_width), BF16),
            pltpu.VMEM((STATE, half_width), BF16),
            pltpu.VMEM((8, tokens), F32),
            pltpu.VMEM((n_tp - 1, 8, tokens), F32),
            pltpu.SemaphoreType.DMA((3, blocks)),
            pltpu.SemaphoreType.DMA((blocks,)),
            pltpu.SemaphoreType.DMA((copies,)),
            pltpu.SemaphoreType.DMA((copies,)),
        ],
        compiler_params=pltpu.CompilerParams(
            collective_id=0, has_side_effects=True, vmem_limit_bytes=60 * 1024 * 1024
        ),
        name="scan",
    )(
        x_input,
        bc_input,
        z_gate,
        dt_input,
        taps(conv_weight_x, conv_bias_x),
        taps(conv_weight_bc, conv_bias_bc),
        head_rows,
    )
    return pl.pallas_call(
        scale_kernel,
        grid=(blocks,),
        out_shape=jax.ShapeDtypeStruct((tokens, width), BF16),
        in_specs=[
            pl.BlockSpec((SPAN, width), lambda i: (i, 0)),
            pl.BlockSpec((8, SPAN), lambda i: (0, i)),
            pl.BlockSpec((1, width), lambda i: (0, 0)),
        ],
        out_specs=pl.BlockSpec((SPAN, width), lambda i: (i, 0)),
        name="scale",
    )(gated, factor, norm_gain[None, :])


def solution(mesh):
    in_specs = (
        P("seq", "tp"),
        P("seq", "tp"),
        P("seq", "tp"),
        P("tp", "seq"),
        P(None, "tp"),
        P(None, "tp"),
        P("tp"),
        P("tp"),
        P("tp"),
        P("tp"),
        P("tp"),
        P("tp"),
    )
    body = functools.partial(local, mesh.shape["seq"], mesh.shape["tp"])
    return jax.shard_map(
        body, mesh=mesh, in_specs=in_specs, out_specs=P("seq", "tp"), check_vma=False
    )
```

```python
import functools

import jax
import jax.numpy as jnp
from jax import lax
from jax.experimental import pallas as pl
from jax.experimental.pallas import tpu as pltpu
from jax.sharding import PartitionSpec as P

HEAD_DIM = 64
STATE = 128
SPAN = 256
LANES = 256
PIECE = 64
RIM = 16
DECAY_ROWS = 16

epsilon = 1e-05

F32 = jnp.float32
BF16 = jnp.bfloat16
MESH = pl.DeviceIdType.MESH


def silu(value):
    half = 0.5 * value
    return half + half * jnp.tanh(half)


def conv_piece(buffer, row, lanes, taps):
    raw = buffer[pl.ds(row, PIECE + RIM), lanes].astype(F32)
    total = raw[RIM - 3 : RIM - 3 + PIECE] * taps[0:1, lanes] + taps[4:5, lanes]
    for k in range(1, 4):
        total = total + raw[RIM - 3 + k : RIM - 3 + k + PIECE] * taps[k : k + 1, lanes]
    return silu(total).astype(BF16)


def two_rows(row):
    high = row.astype(BF16).astype(F32)
    low = row - high
    width = row.shape[1]
    return jnp.concatenate(
        [jnp.broadcast_to(high, (8, width)), jnp.broadcast_to(low, (8, width))], 0
    ).astype(BF16)


def read_row(pair):
    wide = pair.astype(F32)
    return wide[0:1] + wide[8:9]


def scan_kernel(
    n_seq,
    n_tp,
    steps,
    x_hbm,
    bc_hbm,
    z_hbm,
    dt_ref,
    weight_x,
    weight_bc,
    bias_x,
    bias_bc,
    dt_bias,
    decay_log,
    skip_scale,
    gated_hbm,
    total_ref,
    xb,
    bcb,
    zb,
    xc,
    xp,
    bcc,
    tt,
    rn,
    rp,
    dec,
    pre,
    u,
    ls,
    own,
    p_buf,
    q_buf,
    gb,
    sm,
    skip_row,
    sq,
    i_buf,
    e_buf,
    d_buf,
    sa,
    ra,
    sk,
    rk,
    se,
    re,
    ss,
    rs,
    taps_x,
    taps_bc,
    in_sem,
    out_sem,
    send_sem,
    recv_sem,
):
    tokens, width = x_hbm.shape
    heads = dt_ref.shape[0]
    groups = bc_hbm.shape[1] // (2 * STATE)
    group_width = width // groups
    half_width = width // 2
    blocks = tokens // SPAN
    chunks = width // LANES
    quarter = half_width // 2
    quarter_chunks = quarter // LANES
    seq = lax.axis_index("seq")
    tp = lax.axis_index("tp")
    chip, core = seq // 2, seq % 2
    partner = seq + 1 - 2 * core
    chips = n_seq // 2

    def rows_of(b):
        return pl.ds(b * SPAN, SPAN)

    loads = []
    for b in range(blocks):
        loads.append(
            (
                pltpu.make_async_copy(
                    bc_hbm.at[rows_of(b), :],
                    bcb.at[pl.ds(RIM + b * SPAN, SPAN), :],
                    in_sem.at[0, b],
                ),
                pltpu.make_async_copy(
                    x_hbm.at[rows_of(b), :],
                    xb.at[pl.ds(RIM + b * SPAN, SPAN), :],
                    in_sem.at[1, b],
                ),
                pltpu.make_async_copy(z_hbm.at[rows_of(b), :], zb.at[rows_of(b), :], in_sem.at[2, b]),
            )
        )
    for b in range(blocks):
        loads[b][0].start()
        loads[b][1].start()
    for b in range(blocks):
        loads[b][2].start()

    def at_seq(place):
        return {"seq": place, "tp": tp}

    barrier = pltpu.get_barrier_semaphore()
    sources = [at_seq((seq + n_seq - 1) % n_seq), at_seq(partner)]
    for j in range(steps):
        sources.append(at_seq(((chip + chips - 2**j) % chips) * 2 + core))
    for k in range(1, n_tp):
        sources.append({"seq": seq, "tp": (tp + n_tp - k) % n_tp})
    for source in sources:
        pl.semaphore_signal(barrier, inc=1, device_id=source, device_id_type=MESH)
    pl.semaphore_wait(barrier, len(sources))

    def remote(source, target, slot, device):
        return pltpu.make_async_remote_copy(
            src_ref=source,
            dst_ref=target,
            send_sem=send_sem.at[slot],
            recv_sem=recv_sem.at[slot],
            device_id=device,
            device_id_type=MESH,
        )

    following = at_seq((seq + 1) % n_seq)
    last_rows = pl.ds(tokens - RIM, RIM)
    rim_x = remote(x_hbm.at[last_rows, :], xb.at[pl.ds(0, RIM), :], 0, following)
    rim_bc = remote(bc_hbm.at[last_rows, :], bcb.at[pl.ds(0, RIM), :], 1, following)
    rim_x.start()
    rim_bc.start()

    row_id = lax.broadcasted_iota(jnp.int32, (256, LANES), 0) % 128
    lane_id = lax.broadcasted_iota(jnp.int32, (256, LANES), 1) // HEAD_DIM
    for c in range(chunks):
        lanes = pl.ds(c * LANES, LANES)
        head = lane_id + c * (LANES // HEAD_DIM)
        rn[:, lanes] = jnp.where(row_id == head, 1.0, 0.0).astype(BF16)
        rp[:, lanes] = jnp.where(row_id == head + heads, 1.0, 0.0).astype(BF16)
    upper = jnp.where(
        lax.broadcasted_iota(jnp.int32, (SPAN, SPAN), 0)
        <= lax.broadcasted_iota(jnp.int32, (SPAN, SPAN), 1),
        1.0,
        0.0,
    )
    eye = lax.broadcasted_iota(jnp.int32, (heads, heads), 0) == lax.broadcasted_iota(
        jnp.int32, (heads, heads), 1
    )

    def column(row_ref):
        return jnp.sum(jnp.where(eye, row_ref[...], 0.0), axis=1, keepdims=True)

    for target, weight, bias in ((taps_x, weight_x, bias_x), (taps_bc, weight_bc, bias_bc)):
        target[0:4, :] = weight[...].astype(F32)
        target[4:5, :] = bias[...]
    rate = -jnp.exp(column(decay_log))
    shift = column(dt_bias)
    for b in range(blocks):
        raw = dt_ref[:, rows_of(b)].astype(F32) + shift
        step = jnp.maximum(raw, 0.0) + jnp.log(1.0 + jnp.exp(-jnp.abs(raw)))
        cum = jnp.dot(
            rate * step, upper, precision=lax.Precision.HIGHEST, preferred_element_type=F32
        )
        parts = [jnp.exp(-cum) * step, jnp.exp(cum)]
        if 2 * heads < 128:
            parts.append(jnp.zeros((128 - 2 * heads, SPAN), F32))
        turned = jnp.concatenate(parts, 0).T
        high = turned.astype(BF16)
        tt[rows_of(b), 0:128] = high
        tt[rows_of(b), 128:256] = (turned - high.astype(F32)).astype(BF16)
    skip_wide = jnp.broadcast_to(skip_scale[...], (16, heads))
    skip_high = skip_wide.astype(BF16)
    skip_low = (skip_wide - skip_high.astype(F32)).astype(BF16)
    for c in range(chunks):
        lanes = pl.ds(c * LANES, LANES)
        skip_row[:, lanes] = (
            jnp.dot(skip_high, rn[0:heads, lanes], preferred_element_type=F32)
            + jnp.dot(skip_low, rn[0:heads, lanes], preferred_element_type=F32)
        )[0:8]
        running = jnp.ones((1, LANES), F32)
        for b in range(blocks):
            ends = jnp.dot(
                tt[pl.ds((b + 1) * SPAN - 16, 16), :], rp[:, lanes], preferred_element_type=F32
            )
            dec[b : b + 1, lanes] = ends[15:16]
            pre[b : b + 1, lanes] = running
            running = running * ends[15:16]
        pre[blocks : blocks + 1, lanes] = running

    def place_of(stage, c):
        half = c // quarter_chunks
        inside = stage * quarter + (c % quarter_chunks) * LANES
        lanes = pl.ds(pl.multiple_of(half * half_width + inside, LANES), LANES)
        piece = pl.ds(pl.multiple_of((c % quarter_chunks) * LANES, LANES), LANES)
        local = pl.ds(pl.multiple_of(inside, LANES), LANES)
        group = (half * half_width + inside) // group_width
        return half, lanes, piece, local, group

    def conv_block(b, stage):
        def bc_piece(r, carry):
            row = pl.multiple_of(b * SPAN + r * PIECE, PIECE)
            for c in range(2 * groups * STATE // LANES):
                lanes = pl.ds(c * LANES, LANES)
                bcc[pl.ds(row, PIECE), lanes] = conv_piece(bcb, row, lanes, taps_bc)
            return carry

        if stage == 0:
            lax.fori_loop(0, SPAN // PIECE, bc_piece, 0)

        def x_chunk(c, carry):
            _, lanes, _, _, group = place_of(stage, c)
            scale = jnp.dot(tt[rows_of(b), :], rn[:, lanes], preferred_element_type=F32)
            for r in range(SPAN // PIECE):
                row = b * SPAN + r * PIECE
                conv = conv_piece(xb, row, lanes, taps_x)
                xc[pl.ds(row, PIECE), lanes] = conv
                xp[pl.ds(row, PIECE), lanes] = (
                    conv.astype(F32) * scale[r * PIECE : (r + 1) * PIECE]
                ).astype(BF16)
            b_part = bcc[rows_of(b), pl.ds(pl.multiple_of(group * 2 * STATE, STATE), STATE)]
            u[b, :, lanes] = lax.dot_general(
                b_part, xp[rows_of(b), lanes], (((0,), (0,)), ((), ())), preferred_element_type=F32
            )
            return carry

        lax.fori_loop(0, chunks // 2, x_chunk, 0)

    loads[0][0].wait()
    loads[0][1].wait()
    for b in range(1, blocks):
        loads[b][0].wait()
        loads[b][1].wait()
        conv_block(b, 0)
    rim_x.wait()
    rim_bc.wait()
    inner = (seq > 0).astype(F32)
    xb[0:RIM, :] = (xb[0:RIM, :].astype(F32) * inner).astype(BF16)
    bcb[0:RIM, :] = (bcb[0:RIM, :].astype(F32) * inner).astype(BF16)
    conv_block(0, 0)

    def carry_chunk(stage, c, carry):
        half, lanes, piece, _, _ = place_of(stage, c)
        state = jnp.zeros((STATE, LANES), F32)
        for b in range(blocks):
            ls[b, :, lanes] = state.astype(BF16)
            state = dec[b : b + 1, lanes] * (state + u[b, :, lanes])
        own[:, lanes] = state
        sa[stage, half, 0:STATE, piece] = state.astype(BF16)
        sa[stage, half, STATE : STATE + DECAY_ROWS, piece] = two_rows(pre[blocks : blocks + 1, lanes])
        return carry

    def pair(stage):
        return remote(sa.at[stage], ra.at[stage], 2 + stage, at_seq(partner))

    def send_state(stage):
        lax.fori_loop(0, chunks // 2, functools.partial(carry_chunk, stage), 0)
        pair(stage).start()

    causal = lax.broadcasted_iota(jnp.int32, (SPAN, SPAN), 0) >= lax.broadcasted_iota(
        jnp.int32, (SPAN, SPAN), 1
    )

    def intra_block(b):
        loads[b][2].wait()
        for g in range(groups):
            b_part = bcc[rows_of(b), pl.ds(g * 2 * STATE, STATE)]
            c_part = bcc[rows_of(b), pl.ds(g * 2 * STATE + STATE, STATE)]
            scores = lax.dot_general(
                c_part, b_part, (((1,), (1,)), ((), ())), preferred_element_type=F32
            )
            sm[g] = jnp.where(causal, scores, 0.0).astype(BF16)

        def chunk(c, carry):
            lanes = pl.ds(pl.multiple_of(c * LANES, LANES), LANES)
            group = c // (group_width // LANES)
            c_part = bcc[
                rows_of(b), pl.ds(pl.multiple_of(group * 2 * STATE + STATE, STATE), STATE)
            ]
            y = jnp.dot(sm[group], xp[rows_of(b), lanes], preferred_element_type=F32)
            y = y + jnp.dot(c_part, ls[b, :, lanes], preferred_element_type=F32)
            scale = jnp.dot(tt[rows_of(b), :], rp[:, lanes], preferred_element_type=F32)
            for r in range(SPAN // PIECE):
                part = slice(r * PIECE, (r + 1) * PIECE)
                rows = pl.ds(b * SPAN + r * PIECE, PIECE)
                gate = silu(zb[rows, lanes].astype(F32))
                mixed = scale[part] * y[part] + skip_row[0:1, lanes] * xc[rows, lanes].astype(F32)
                p_buf[rows, lanes] = mixed * gate
                q_buf[rows, lanes] = scale[part] * gate
            return carry

        lax.fori_loop(0, chunks, chunk, 0)

    flag = core.astype(F32)

    def joined_chunk(stage, j, carry):
        piece = pl.ds(pl.multiple_of(j * LANES, LANES), LANES)
        inside = stage * quarter + j * LANES
        local = pl.ds(pl.multiple_of(inside, LANES), LANES)
        lanes = pl.ds(pl.multiple_of(core * half_width + inside, LANES), LANES)
        mine, mine_decay = own[:, lanes], pre[blocks : blocks + 1, lanes]
        other = ra[stage, core, 0:STATE, piece].astype(F32)
        other_decay = read_row(ra[stage, core, STATE : STATE + DECAY_ROWS, piece])
        joined = (1.0 - flag) * (other_decay * mine + other) + flag * (mine_decay * other + mine)
        decay = mine_decay * other_decay
        i_buf[:, local] = joined
        e_buf[:, local] = jnp.zeros_like(joined)
        d_buf[0:1, local] = decay
        d_buf[1:2, local] = jnp.ones_like(decay)
        sk[stage, 0, 0:STATE, piece] = joined.astype(BF16)
        sk[stage, 0, STATE : STATE + DECAY_ROWS, piece] = two_rows(decay)
        return carry

    def double(stage, step):
        valid = (chip >= 2**step).astype(F32)

        def body(j, carry):
            piece = pl.ds(pl.multiple_of(j * LANES, LANES), LANES)
            local = pl.ds(pl.multiple_of(stage * quarter + j * LANES, LANES), LANES)
            got = rk[stage, step, 0:STATE, piece].astype(F32) * valid
            got_decay = (
                read_row(rk[stage, step, STATE : STATE + DECAY_ROWS, piece]) * valid + (1.0 - valid)
            )
            e_decay = d_buf[1:2, local]
            earlier = e_decay * got + e_buf[:, local]
            e_buf[:, local] = earlier
            d_buf[1:2, local] = e_decay * got_decay
            if step < steps - 1:
                i_decay = d_buf[0:1, local]
                joined = i_decay * got + i_buf[:, local]
                decay = i_decay * got_decay
                i_buf[:, local] = joined
                d_buf[0:1, local] = decay
                sk[stage, step + 1, 0:STATE, piece] = joined.astype(BF16)
                sk[stage, step + 1, STATE : STATE + DECAY_ROWS, piece] = two_rows(decay)
            else:
                se[stage, :, piece] = earlier.astype(BF16)
            return carry

        lax.fori_loop(0, quarter_chunks, body, 0)

    def hop(stage, step):
        target = at_seq(((chip + 2**step) % chips) * 2 + core)
        slot = 6 + stage * steps + step
        return remote(sk.at[stage, step], rk.at[stage, step], slot, target)

    def back(stage):
        return remote(se.at[stage], re.at[stage], 4 + stage, at_seq(partner))

    def join_pair(stage):
        pair(stage).wait()
        lax.fori_loop(0, quarter_chunks, functools.partial(joined_chunk, stage), 0)
        hop(stage, 0).start()

    def advance(stage, step):
        hop(stage, step).wait()
        double(stage, step)
        if step < steps - 1:
            hop(stage, step + 1).start()
        else:
            back(stage).start()

    def incoming_chunk(stage, c, carry):
        half, lanes, piece, local, _ = place_of(stage, c)
        here = (half == core).astype(F32)
        state = here * e_buf[:, local] + (1.0 - here) * re[stage, :, piece].astype(F32)
        other = ra[stage, half, 0:STATE, piece].astype(F32)
        other_decay = read_row(ra[stage, half, STATE : STATE + DECAY_ROWS, piece])
        own[:, lanes] = (1.0 - flag) * state + flag * (other_decay * state + other)
        return carry

    stores = []

    def final_block(b, stage):
        if stage == 0:
            sq[rows_of(b), :] = jnp.zeros((SPAN, 128), F32)

        def final(c, carry):
            _, lanes, _, _, group = place_of(stage, c)
            c_part = bcc[
                rows_of(b), pl.ds(pl.multiple_of(group * 2 * STATE + STATE, STATE), STATE)
            ]
            start = (own[:, lanes] * pre[b : b + 1, lanes]).astype(BF16)
            y = jnp.dot(c_part, start, preferred_element_type=F32)
            for r in range(SPAN // PIECE):
                part = slice(r * PIECE, (r + 1) * PIECE)
                rows = pl.ds(b * SPAN + r * PIECE, PIECE)
                gated = p_buf[rows, lanes] + q_buf[rows, lanes] * y[part]
                gb[rows, lanes] = gated.astype(BF16)
                square = gated * gated
                total = square[:, 0:128]
                for i in range(1, LANES // 128):
                    total = total + square[:, i * 128 : (i + 1) * 128]
                sq[rows, :] += total
            return carry

        lax.fori_loop(0, chunks // 2, final, 0)
        if stage == 1:
            ss[:, rows_of(b)] = jnp.broadcast_to(
                jnp.sum(sq[rows_of(b), :].T, axis=0, keepdims=True), (8, SPAN)
            )
            store = pltpu.make_async_copy(
                gb.at[rows_of(b), :], gated_hbm.at[rows_of(b), :], out_sem.at[b]
            )
            store.start()
            stores.append(store)

    def finish(stage):
        back(stage).wait()
        lax.fori_loop(0, chunks // 2, functools.partial(incoming_chunk, stage), 0)
        for b in range(blocks):
            final_block(b, stage)

    send_state(0)
    conv_block(0, 1)
    join_pair(0)
    for b in range(1, blocks):
        conv_block(b, 1)
    advance(0, 0)
    send_state(1)
    intra_block(0)
    join_pair(1)
    for b in range(1, blocks):
        intra_block(b)
        if b == 1:
            for step in range(1, steps):
                advance(0, step)
        if b == 2:
            advance(1, 0)
    finish(0)
    for step in range(1, steps):
        advance(1, step)
    finish(1)

    shares = []
    for k in range(1, n_tp):
        share = remote(
            ss, rs.at[k - 1], 5 + 2 * steps + k, {"seq": seq, "tp": (tp + k) % n_tp}
        )
        share.start()
        shares.append(share)
    for share in shares:
        share.wait()
    total = ss[...]
    for k in range(n_tp - 1):
        total = total + rs[k]
    total_ref[...] = lax.rsqrt(total * (1.0 / (width * n_tp)) + epsilon)
    for store in stores:
        store.wait()


def scale_kernel(gated_ref, factor_ref, gain_ref, out_ref):
    column = factor_ref[...].T[:, 0:1]
    for r in range(0, gated_ref.shape[0], PIECE):
        rows = pl.ds(r, PIECE)
        wide = gated_ref[rows, :].astype(F32)
        out_ref[rows, :] = (wide * column[r : r + PIECE] * gain_ref[...]).astype(BF16)


def local(
    n_seq,
    n_tp,
    x_input,
    bc_input,
    z_gate,
    dt_input,
    conv_weight_x,
    conv_weight_bc,
    conv_bias_x,
    conv_bias_bc,
    dt_bias,
    decay_log,
    skip_scale,
    norm_gain,
):
    tokens, width = x_input.shape
    bc_width = bc_input.shape[1]
    heads = dt_input.shape[0]
    groups = bc_width // (2 * STATE)
    blocks = tokens // SPAN
    quarter = width // 4
    steps = max(1, (n_seq // 2 - 1).bit_length())

    whole = pl.BlockSpec(memory_space=pltpu.VMEM)
    anywhere = pl.BlockSpec(memory_space=pl.ANY)
    message = STATE + DECAY_ROWS
    copies = 6 + 2 * steps + n_tp - 1
    gated, factor = pl.pallas_call(
        functools.partial(scan_kernel, n_seq, n_tp, steps),
        out_shape=(
            jax.ShapeDtypeStruct((tokens, width), BF16),
            jax.ShapeDtypeStruct((8, tokens), F32),
        ),
        in_specs=[anywhere] * 3 + [whole] * 8,
        out_specs=(anywhere, whole),
        scratch_shapes=[
            pltpu.VMEM((RIM + tokens, width), BF16),
            pltpu.VMEM((RIM + tokens, bc_width), BF16),
            pltpu.VMEM((tokens, width), BF16),
            pltpu.VMEM((tokens, width), BF16),
            pltpu.VMEM((tokens, width), BF16),
            pltpu.VMEM((tokens, bc_width), BF16),
            pltpu.VMEM((tokens, 256), BF16),
            pltpu.VMEM((256, width), BF16),
            pltpu.VMEM((256, width), BF16),
            pltpu.VMEM((8, width), F32),
            pltpu.VMEM((8, width), F32),
            pltpu.VMEM((blocks, STATE, width), F32),
            pltpu.VMEM((blocks, STATE, width), BF16),
            pltpu.VMEM((STATE, width), F32),
            pltpu.VMEM((tokens, width), F32),
            pltpu.VMEM((tokens, width), F32),
            pltpu.VMEM((tokens, width), BF16),
            pltpu.VMEM((groups, SPAN, SPAN), BF16),
            pltpu.VMEM((8, width), F32),
            pltpu.VMEM((tokens, 128), F32),
            pltpu.VMEM((STATE, 2 * quarter), F32),
            pltpu.VMEM((STATE, 2 * quarter), F32),
            pltpu.VMEM((8, 2 * quarter), F32),
            pltpu.VMEM((2, 2, message, quarter), BF16),
            pltpu.VMEM((2, 2, message, quarter), BF16),
            pltpu.VMEM((2, steps, message, quarter), BF16),
            pltpu.VMEM((2, steps, message, quarter), BF16),
            pltpu.VMEM((2, STATE, quarter), BF16),
            pltpu.VMEM((2, STATE, quarter), BF16),
            pltpu.VMEM((8, tokens), F32),
            pltpu.VMEM((n_tp - 1, 8, tokens), F32),
            pltpu.VMEM((8, width), F32),
            pltpu.VMEM((8, bc_width), F32),
            pltpu.SemaphoreType.DMA((3, blocks)),
            pltpu.SemaphoreType.DMA((blocks,)),
            pltpu.SemaphoreType.DMA((copies,)),
            pltpu.SemaphoreType.DMA((copies,)),
        ],
        compiler_params=pltpu.CompilerParams(
            collective_id=0, has_side_effects=True, vmem_limit_bytes=60 * 1024 * 1024
        ),
        name="scan",
    )(
        x_input,
        bc_input,
        z_gate,
        dt_input,
        conv_weight_x,
        conv_weight_bc,
        conv_bias_x[None, :],
        conv_bias_bc[None, :],
        dt_bias[None, :],
        decay_log[None, :],
        skip_scale[None, :],
    )
    return pl.pallas_call(
        scale_kernel,
        grid=(blocks,),
        out_shape=jax.ShapeDtypeStruct((tokens, width), BF16),
        in_specs=[
            pl.BlockSpec((SPAN, width), lambda i: (i, 0)),
            pl.BlockSpec((8, SPAN), lambda i: (0, i)),
            pl.BlockSpec((1, width), lambda i: (0, 0)),
        ],
        out_specs=pl.BlockSpec((SPAN, width), lambda i: (i, 0)),
        name="scale",
    )(gated, factor, norm_gain[None, :])


def solution(mesh):
    in_specs = (
        P("seq", "tp"),
        P("seq", "tp"),
        P("seq", "tp"),
        P("tp", "seq"),
        P(None, "tp"),
        P(None, "tp"),
        P("tp"),
        P("tp"),
        P("tp"),
        P("tp"),
        P("tp"),
        P("tp"),
    )
    body = functools.partial(local, mesh.shape["seq"], mesh.shape["tp"])
    return jax.shard_map(
        body, mesh=mesh, in_specs=in_specs, out_specs=P("seq", "tp"), check_vma=False
    )
```

```python
import functools

import jax
import jax.numpy as jnp
from jax import lax
from jax.experimental import pallas as pl
from jax.experimental.pallas import tpu as pltpu
from jax.sharding import PartitionSpec as P

HEAD_DIM = 64
STATE = 128
SPAN = 256
LANES = 256
PIECE = 64
RIM = 16
DECAY_ROWS = 16

epsilon = 1e-05

F32 = jnp.float32
BF16 = jnp.bfloat16
MESH = pl.DeviceIdType.MESH


def silu(value):
    half = 0.5 * value
    return half + half * jnp.tanh(half)


def conv_piece(buffer, row, lanes, taps, shifted):
    raw = buffer[pl.ds(row, PIECE + RIM), lanes].astype(F32)
    bias = taps[4:5, lanes]
    pieces = []
    for i in range(LANES // 128):
        part = slice(i * 128, (i + 1) * 128)
        shifted[i, :, :] = raw[:, part]
        total = raw[RIM:, part] * taps[3:4, lanes][:, part] + bias[:, part]
        for k in range(3):
            tap = taps[k : k + 1, lanes][:, part]
            total = total + shifted[i, pl.ds(RIM - 3 + k, PIECE), :] * tap
        pieces.append(silu(total).astype(BF16))
    return jnp.concatenate(pieces, 1)


def two_rows(row):
    high = row.astype(BF16).astype(F32)
    low = row - high
    width = row.shape[1]
    return jnp.concatenate(
        [jnp.broadcast_to(high, (8, width)), jnp.broadcast_to(low, (8, width))], 0
    ).astype(BF16)


def read_row(pair):
    wide = pair.astype(F32)
    return wide[0:1] + wide[8:9]


def scan_kernel(
    n_seq,
    n_tp,
    steps,
    x_hbm,
    bc_hbm,
    z_hbm,
    dt_ref,
    weight_x,
    weight_bc,
    bias_x,
    bias_bc,
    dt_bias,
    decay_log,
    skip_scale,
    gated_hbm,
    total_ref,
    xb,
    bcb,
    zb,
    xc,
    xp,
    bcc,
    tt,
    rn,
    rp,
    dec,
    pre,
    u,
    ls,
    own,
    p_buf,
    q_buf,
    gb,
    sm,
    skip_row,
    sq,
    i_buf,
    e_buf,
    d_buf,
    sa,
    ra,
    sk,
    rk,
    se,
    re,
    ss,
    rs,
    taps_x,
    taps_bc,
    shifted,
    in_sem,
    out_sem,
    send_sem,
    recv_sem,
):
    tokens, width = x_hbm.shape
    heads = dt_ref.shape[0]
    groups = bc_hbm.shape[1] // (2 * STATE)
    group_width = width // groups
    half_width = width // 2
    blocks = tokens // SPAN
    chunks = width // LANES
    quarter = half_width // 2
    quarter_chunks = quarter // LANES
    seq = lax.axis_index("seq")
    tp = lax.axis_index("tp")
    chip, core = seq // 2, seq % 2
    partner = seq + 1 - 2 * core
    chips = n_seq // 2

    def rows_of(b):
        return pl.ds(b * SPAN, SPAN)

    loads = []
    for b in range(blocks):
        loads.append(
            (
                pltpu.make_async_copy(
                    bc_hbm.at[rows_of(b), :],
                    bcb.at[pl.ds(RIM + b * SPAN, SPAN), :],
                    in_sem.at[0, b],
                ),
                pltpu.make_async_copy(
                    x_hbm.at[rows_of(b), :],
                    xb.at[pl.ds(RIM + b * SPAN, SPAN), :],
                    in_sem.at[1, b],
                ),
                pltpu.make_async_copy(z_hbm.at[rows_of(b), :], zb.at[rows_of(b), :], in_sem.at[2, b]),
            )
        )
    for b in range(blocks):
        loads[b][0].start()
        loads[b][1].start()
    for b in range(blocks):
        loads[b][2].start()

    def at_seq(place):
        return {"seq": place, "tp": tp}

    barrier = pltpu.get_barrier_semaphore()
    sources = [at_seq((seq + n_seq - 1) % n_seq), at_seq(partner)]
    for j in range(steps):
        sources.append(at_seq(((chip + chips - 2**j) % chips) * 2 + core))
    for k in range(1, n_tp):
        sources.append({"seq": seq, "tp": (tp + n_tp - k) % n_tp})
    for source in sources:
        pl.semaphore_signal(barrier, inc=1, device_id=source, device_id_type=MESH)
    pl.semaphore_wait(barrier, len(sources))

    def remote(source, target, slot, device):
        return pltpu.make_async_remote_copy(
            src_ref=source,
            dst_ref=target,
            send_sem=send_sem.at[slot],
            recv_sem=recv_sem.at[slot],
            device_id=device,
            device_id_type=MESH,
        )

    following = at_seq((seq + 1) % n_seq)
    last_rows = pl.ds(tokens - RIM, RIM)
    rim_x = remote(x_hbm.at[last_rows, :], xb.at[pl.ds(0, RIM), :], 0, following)
    rim_bc = remote(bc_hbm.at[last_rows, :], bcb.at[pl.ds(0, RIM), :], 1, following)
    rim_x.start()
    rim_bc.start()

    row_id = lax.broadcasted_iota(jnp.int32, (256, LANES), 0) % 128
    lane_id = lax.broadcasted_iota(jnp.int32, (256, LANES), 1) // HEAD_DIM
    for c in range(chunks):
        lanes = pl.ds(c * LANES, LANES)
        head = lane_id + c * (LANES // HEAD_DIM)
        rn[:, lanes] = jnp.where(row_id == head, 1.0, 0.0).astype(BF16)
        rp[:, lanes] = jnp.where(row_id == head + heads, 1.0, 0.0).astype(BF16)
    upper = jnp.where(
        lax.broadcasted_iota(jnp.int32, (SPAN, SPAN), 0)
        <= lax.broadcasted_iota(jnp.int32, (SPAN, SPAN), 1),
        1.0,
        0.0,
    )
    eye = lax.broadcasted_iota(jnp.int32, (heads, heads), 0) == lax.broadcasted_iota(
        jnp.int32, (heads, heads), 1
    )

    def column(row_ref):
        return jnp.sum(jnp.where(eye, row_ref[...], 0.0), axis=1, keepdims=True)

    for target, weight, bias in ((taps_x, weight_x, bias_x), (taps_bc, weight_bc, bias_bc)):
        target[0:4, :] = weight[...].astype(F32)
        target[4:5, :] = bias[...]
    rate = -jnp.exp(column(decay_log))
    shift = column(dt_bias)
    for b in range(blocks):
        raw = dt_ref[:, rows_of(b)].astype(F32) + shift
        step = jnp.maximum(raw, 0.0) + jnp.log(1.0 + jnp.exp(-jnp.abs(raw)))
        cum = jnp.dot(
            rate * step, upper, precision=lax.Precision.HIGHEST, preferred_element_type=F32
        )
        parts = [jnp.exp(-cum) * step, jnp.exp(cum)]
        if 2 * heads < 128:
            parts.append(jnp.zeros((128 - 2 * heads, SPAN), F32))
        turned = jnp.concatenate(parts, 0).T
        high = turned.astype(BF16)
        tt[rows_of(b), 0:128] = high
        tt[rows_of(b), 128:256] = (turned - high.astype(F32)).astype(BF16)
    skip_wide = jnp.broadcast_to(skip_scale[...], (16, heads))
    skip_high = skip_wide.astype(BF16)
    skip_low = (skip_wide - skip_high.astype(F32)).astype(BF16)
    for c in range(chunks):
        lanes = pl.ds(c * LANES, LANES)
        skip_row[:, lanes] = (
            jnp.dot(skip_high, rn[0:heads, lanes], preferred_element_type=F32)
            + jnp.dot(skip_low, rn[0:heads, lanes], preferred_element_type=F32)
        )[0:8]
        running = jnp.ones((1, LANES), F32)
        for b in range(blocks):
            ends = jnp.dot(
                tt[pl.ds((b + 1) * SPAN - 16, 16), :], rp[:, lanes], preferred_element_type=F32
            )
            dec[b : b + 1, lanes] = ends[15:16]
            pre[b : b + 1, lanes] = running
            running = running * ends[15:16]
        pre[blocks : blocks + 1, lanes] = running

    def place_of(stage, c):
        half = c // quarter_chunks
        inside = stage * quarter + (c % quarter_chunks) * LANES
        lanes = pl.ds(pl.multiple_of(half * half_width + inside, LANES), LANES)
        piece = pl.ds(pl.multiple_of((c % quarter_chunks) * LANES, LANES), LANES)
        local = pl.ds(pl.multiple_of(inside, LANES), LANES)
        group = (half * half_width + inside) // group_width
        return half, lanes, piece, local, group

    def conv_block(b, stage):
        def bc_piece(r, carry):
            row = pl.multiple_of(b * SPAN + r * PIECE, PIECE)
            for c in range(2 * groups * STATE // LANES):
                lanes = pl.ds(c * LANES, LANES)
                bcc[pl.ds(row, PIECE), lanes] = conv_piece(
                    bcb, row, lanes, taps_bc, shifted.at[c % 2]
                )
            return carry

        if stage == 0:
            lax.fori_loop(0, SPAN // PIECE, bc_piece, 0)

        def x_chunk(c, carry):
            _, lanes, _, _, group = place_of(stage, c)
            scale = jnp.dot(tt[rows_of(b), :], rn[:, lanes], preferred_element_type=F32)
            for r in range(SPAN // PIECE):
                row = b * SPAN + r * PIECE
                conv = conv_piece(xb, row, lanes, taps_x, shifted.at[r % 2])
                xc[pl.ds(row, PIECE), lanes] = conv
                xp[pl.ds(row, PIECE), lanes] = (
                    conv.astype(F32) * scale[r * PIECE : (r + 1) * PIECE]
                ).astype(BF16)
            b_part = bcc[rows_of(b), pl.ds(pl.multiple_of(group * 2 * STATE, STATE), STATE)]
            u[b, :, lanes] = lax.dot_general(
                b_part, xp[rows_of(b), lanes], (((0,), (0,)), ((), ())), preferred_element_type=F32
            )
            return carry

        lax.fori_loop(0, chunks // 2, x_chunk, 0)

    loads[0][0].wait()
    loads[0][1].wait()
    for b in range(1, blocks):
        loads[b][0].wait()
        loads[b][1].wait()
        conv_block(b, 0)
    rim_x.wait()
    rim_bc.wait()
    inner = (seq > 0).astype(F32)
    xb[0:RIM, :] = (xb[0:RIM, :].astype(F32) * inner).astype(BF16)
    bcb[0:RIM, :] = (bcb[0:RIM, :].astype(F32) * inner).astype(BF16)
    conv_block(0, 0)

    def carry_chunk(stage, c, carry):
        half, lanes, piece, _, _ = place_of(stage, c)
        state = jnp.zeros((STATE, LANES), F32)
        for b in range(blocks):
            ls[b, :, lanes] = state.astype(BF16)
            state = dec[b : b + 1, lanes] * (state + u[b, :, lanes])
        own[:, lanes] = state
        sa[stage, half, 0:STATE, piece] = state.astype(BF16)
        sa[stage, half, STATE : STATE + DECAY_ROWS, piece] = two_rows(pre[blocks : blocks + 1, lanes])
        return carry

    def pair(stage):
        return remote(sa.at[stage], ra.at[stage], 2 + stage, at_seq(partner))

    def send_state(stage):
        lax.fori_loop(0, chunks // 2, functools.partial(carry_chunk, stage), 0)
        pair(stage).start()

    causal = lax.broadcasted_iota(jnp.int32, (SPAN, SPAN), 0) >= lax.broadcasted_iota(
        jnp.int32, (SPAN, SPAN), 1
    )

    def intra_block(b):
        loads[b][2].wait()
        for g in range(groups):
            b_part = bcc[rows_of(b), pl.ds(g * 2 * STATE, STATE)]
            c_part = bcc[rows_of(b), pl.ds(g * 2 * STATE + STATE, STATE)]
            scores = lax.dot_general(
                c_part, b_part, (((1,), (1,)), ((), ())), preferred_element_type=F32
            )
            sm[g] = jnp.where(causal, scores, 0.0).astype(BF16)

        def chunk(c, carry):
            lanes = pl.ds(pl.multiple_of(c * LANES, LANES), LANES)
            group = c // (group_width // LANES)
            c_part = bcc[
                rows_of(b), pl.ds(pl.multiple_of(group * 2 * STATE + STATE, STATE), STATE)
            ]
            y = jnp.dot(sm[group], xp[rows_of(b), lanes], preferred_element_type=F32)
            y = y + jnp.dot(c_part, ls[b, :, lanes], preferred_element_type=F32)
            scale = jnp.dot(tt[rows_of(b), :], rp[:, lanes], preferred_element_type=F32)
            for r in range(SPAN // PIECE):
                part = slice(r * PIECE, (r + 1) * PIECE)
                rows = pl.ds(b * SPAN + r * PIECE, PIECE)
                gate = silu(zb[rows, lanes].astype(F32))
                mixed = scale[part] * y[part] + skip_row[0:1, lanes] * xc[rows, lanes].astype(F32)
                p_buf[rows, lanes] = mixed * gate
                q_buf[rows, lanes] = scale[part] * gate
            return carry

        lax.fori_loop(0, chunks, chunk, 0)

    flag = core.astype(F32)

    def joined_chunk(stage, j, carry):
        piece = pl.ds(pl.multiple_of(j * LANES, LANES), LANES)
        inside = stage * quarter + j * LANES
        local = pl.ds(pl.multiple_of(inside, LANES), LANES)
        lanes = pl.ds(pl.multiple_of(core * half_width + inside, LANES), LANES)
        mine, mine_decay = own[:, lanes], pre[blocks : blocks + 1, lanes]
        other = ra[stage, core, 0:STATE, piece].astype(F32)
        other_decay = read_row(ra[stage, core, STATE : STATE + DECAY_ROWS, piece])
        joined = (1.0 - flag) * (other_decay * mine + other) + flag * (mine_decay * other + mine)
        decay = mine_decay * other_decay
        i_buf[:, local] = joined
        e_buf[:, local] = jnp.zeros_like(joined)
        d_buf[0:1, local] = decay
        d_buf[1:2, local] = jnp.ones_like(decay)
        sk[stage, 0, 0:STATE, piece] = joined.astype(BF16)
        sk[stage, 0, STATE : STATE + DECAY_ROWS, piece] = two_rows(decay)
        return carry

    def double(stage, step):
        valid = (chip >= 2**step).astype(F32)

        def body(j, carry):
            piece = pl.ds(pl.multiple_of(j * LANES, LANES), LANES)
            local = pl.ds(pl.multiple_of(stage * quarter + j * LANES, LANES), LANES)
            got = rk[stage, step, 0:STATE, piece].astype(F32) * valid
            got_decay = (
                read_row(rk[stage, step, STATE : STATE + DECAY_ROWS, piece]) * valid + (1.0 - valid)
            )
            e_decay = d_buf[1:2, local]
            earlier = e_decay * got + e_buf[:, local]
            e_buf[:, local] = earlier
            d_buf[1:2, local] = e_decay * got_decay
            if step < steps - 1:
                i_decay = d_buf[0:1, local]
                joined = i_decay * got + i_buf[:, local]
                decay = i_decay * got_decay
                i_buf[:, local] = joined
                d_buf[0:1, local] = decay
                sk[stage, step + 1, 0:STATE, piece] = joined.astype(BF16)
                sk[stage, step + 1, STATE : STATE + DECAY_ROWS, piece] = two_rows(decay)
            else:
                se[stage, :, piece] = earlier.astype(BF16)
            return carry

        lax.fori_loop(0, quarter_chunks, body, 0)

    def hop(stage, step):
        target = at_seq(((chip + 2**step) % chips) * 2 + core)
        slot = 6 + stage * steps + step
        return remote(sk.at[stage, step], rk.at[stage, step], slot, target)

    def back(stage):
        return remote(se.at[stage], re.at[stage], 4 + stage, at_seq(partner))

    def join_pair(stage):
        pair(stage).wait()
        lax.fori_loop(0, quarter_chunks, functools.partial(joined_chunk, stage), 0)
        hop(stage, 0).start()

    def advance(stage, step):
        hop(stage, step).wait()
        double(stage, step)
        if step < steps - 1:
            hop(stage, step + 1).start()
        else:
            back(stage).start()

    def incoming_chunk(stage, c, carry):
        half, lanes, piece, local, _ = place_of(stage, c)
        here = (half == core).astype(F32)
        state = here * e_buf[:, local] + (1.0 - here) * re[stage, :, piece].astype(F32)
        other = ra[stage, half, 0:STATE, piece].astype(F32)
        other_decay = read_row(ra[stage, half, STATE : STATE + DECAY_ROWS, piece])
        own[:, lanes] = (1.0 - flag) * state + flag * (other_decay * state + other)
        return carry

    stores = []

    def final_block(b, stage):
        if stage == 0:
            sq[rows_of(b), :] = jnp.zeros((SPAN, 128), F32)

        def final(c, carry):
            _, lanes, _, _, group = place_of(stage, c)
            c_part = bcc[
                rows_of(b), pl.ds(pl.multiple_of(group * 2 * STATE + STATE, STATE), STATE)
            ]
            start = (own[:, lanes] * pre[b : b + 1, lanes]).astype(BF16)
            y = jnp.dot(c_part, start, preferred_element_type=F32)
            for r in range(SPAN // PIECE):
                part = slice(r * PIECE, (r + 1) * PIECE)
                rows = pl.ds(b * SPAN + r * PIECE, PIECE)
                gated = p_buf[rows, lanes] + q_buf[rows, lanes] * y[part]
                gb[rows, lanes] = gated.astype(BF16)
                square = gated * gated
                total = square[:, 0:128]
                for i in range(1, LANES // 128):
                    total = total + square[:, i * 128 : (i + 1) * 128]
                sq[rows, :] += total
            return carry

        lax.fori_loop(0, chunks // 2, final, 0)
        if stage == 1:
            ss[:, rows_of(b)] = jnp.broadcast_to(
                jnp.sum(sq[rows_of(b), :].T, axis=0, keepdims=True), (8, SPAN)
            )
            store = pltpu.make_async_copy(
                gb.at[rows_of(b), :], gated_hbm.at[rows_of(b), :], out_sem.at[b]
            )
            store.start()
            stores.append(store)

    def finish(stage):
        back(stage).wait()
        lax.fori_loop(0, chunks // 2, functools.partial(incoming_chunk, stage), 0)
        for b in range(blocks):
            final_block(b, stage)

    send_state(0)
    conv_block(0, 1)
    join_pair(0)
    for b in range(1, blocks):
        conv_block(b, 1)
    advance(0, 0)
    send_state(1)
    intra_block(0)
    join_pair(1)
    for b in range(1, blocks):
        intra_block(b)
        if b == 1:
            for step in range(1, steps):
                advance(0, step)
        if b == 2:
            advance(1, 0)
    finish(0)
    for step in range(1, steps):
        advance(1, step)
    finish(1)

    shares = []
    for k in range(1, n_tp):
        share = remote(
            ss, rs.at[k - 1], 5 + 2 * steps + k, {"seq": seq, "tp": (tp + k) % n_tp}
        )
        share.start()
        shares.append(share)
    for share in shares:
        share.wait()
    total = ss[...]
    for k in range(n_tp - 1):
        total = total + rs[k]
    total_ref[...] = lax.rsqrt(total * (1.0 / (width * n_tp)) + epsilon)
    for store in stores:
        store.wait()


def scale_kernel(gated_ref, factor_ref, gain_ref, out_ref):
    column = factor_ref[...].T[:, 0:1]
    for r in range(0, gated_ref.shape[0], PIECE):
        rows = pl.ds(r, PIECE)
        wide = gated_ref[rows, :].astype(F32)
        out_ref[rows, :] = (wide * column[r : r + PIECE] * gain_ref[...]).astype(BF16)


def local(
    n_seq,
    n_tp,
    x_input,
    bc_input,
    z_gate,
    dt_input,
    conv_weight_x,
    conv_weight_bc,
    conv_bias_x,
    conv_bias_bc,
    dt_bias,
    decay_log,
    skip_scale,
    norm_gain,
):
    tokens, width = x_input.shape
    bc_width = bc_input.shape[1]
    heads = dt_input.shape[0]
    groups = bc_width // (2 * STATE)
    blocks = tokens // SPAN
    quarter = width // 4
    steps = max(1, (n_seq // 2 - 1).bit_length())

    whole = pl.BlockSpec(memory_space=pltpu.VMEM)
    anywhere = pl.BlockSpec(memory_space=pl.ANY)
    message = STATE + DECAY_ROWS
    copies = 6 + 2 * steps + n_tp - 1
    gated, factor = pl.pallas_call(
        functools.partial(scan_kernel, n_seq, n_tp, steps),
        out_shape=(
            jax.ShapeDtypeStruct((tokens, width), BF16),
            jax.ShapeDtypeStruct((8, tokens), F32),
        ),
        in_specs=[anywhere] * 3 + [whole] * 8,
        out_specs=(anywhere, whole),
        scratch_shapes=[
            pltpu.VMEM((RIM + tokens, width), BF16),
            pltpu.VMEM((RIM + tokens, bc_width), BF16),
            pltpu.VMEM((tokens, width), BF16),
            pltpu.VMEM((tokens, width), BF16),
            pltpu.VMEM((tokens, width), BF16),
            pltpu.VMEM((tokens, bc_width), BF16),
            pltpu.VMEM((tokens, 256), BF16),
            pltpu.VMEM((256, width), BF16),
            pltpu.VMEM((256, width), BF16),
            pltpu.VMEM((8, width), F32),
            pltpu.VMEM((8, width), F32),
            pltpu.VMEM((blocks, STATE, width), F32),
            pltpu.VMEM((blocks, STATE, width), BF16),
            pltpu.VMEM((STATE, width), F32),
            pltpu.VMEM((tokens, width), F32),
            pltpu.VMEM((tokens, width), F32),
            pltpu.VMEM((tokens, width), BF16),
            pltpu.VMEM((groups, SPAN, SPAN), BF16),
            pltpu.VMEM((8, width), F32),
            pltpu.VMEM((tokens, 128), F32),
            pltpu.VMEM((STATE, 2 * quarter), F32),
            pltpu.VMEM((STATE, 2 * quarter), F32),
            pltpu.VMEM((8, 2 * quarter), F32),
            pltpu.VMEM((2, 2, message, quarter), BF16),
            pltpu.VMEM((2, 2, message, quarter), BF16),
            pltpu.VMEM((2, steps, message, quarter), BF16),
            pltpu.VMEM((2, steps, message, quarter), BF16),
            pltpu.VMEM((2, STATE, quarter), BF16),
            pltpu.VMEM((2, STATE, quarter), BF16),
            pltpu.VMEM((8, tokens), F32),
            pltpu.VMEM((n_tp - 1, 8, tokens), F32),
            pltpu.VMEM((8, width), F32),
            pltpu.VMEM((8, bc_width), F32),
            pltpu.VMEM((2, LANES // 128, PIECE + RIM, 128), F32),
            pltpu.SemaphoreType.DMA((3, blocks)),
            pltpu.SemaphoreType.DMA((blocks,)),
            pltpu.SemaphoreType.DMA((copies,)),
            pltpu.SemaphoreType.DMA((copies,)),
        ],
        compiler_params=pltpu.CompilerParams(
            collective_id=0, has_side_effects=True, vmem_limit_bytes=60 * 1024 * 1024
        ),
        name="scan",
    )(
        x_input,
        bc_input,
        z_gate,
        dt_input,
        conv_weight_x,
        conv_weight_bc,
        conv_bias_x[None, :],
        conv_bias_bc[None, :],
        dt_bias[None, :],
        decay_log[None, :],
        skip_scale[None, :],
    )
    return pl.pallas_call(
        scale_kernel,
        grid=(2 * blocks,),
        out_shape=jax.ShapeDtypeStruct((tokens, width), BF16),
        in_specs=[
            pl.BlockSpec((SPAN // 2, width), lambda i: (i, 0)),
            pl.BlockSpec((8, SPAN // 2), lambda i: (0, i)),
            pl.BlockSpec((1, width), lambda i: (0, 0)),
        ],
        out_specs=pl.BlockSpec((SPAN // 2, width), lambda i: (i, 0)),
        name="scale",
    )(gated, factor, norm_gain[None, :])


def solution(mesh):
    in_specs = (
        P("seq", "tp"),
        P("seq", "tp"),
        P("seq", "tp"),
        P("tp", "seq"),
        P(None, "tp"),
        P(None, "tp"),
        P("tp"),
        P("tp"),
        P("tp"),
        P("tp"),
        P("tp"),
        P("tp"),
    )
    body = functools.partial(local, mesh.shape["seq"], mesh.shape["tp"])
    return jax.shard_map(
        body, mesh=mesh, in_specs=in_specs, out_specs=P("seq", "tp"), check_vma=False
    )
```
